32 devices in a mesh: pp: 2 (over core), ep: 16 (over z, y, x), tp: 1.
Axes of the slice: x: 2, y: 2, z: 4, core: 2. Of those that a mesh axis runs over, the one named last changes fastest.
Arguments:
- acts: bfloat16 [2, 96, 3072], P(None, 'ep'), may hold values from -6 to 6
- route_ids: int32 [2, 2, 96, 8], P('pp', None, 'ep'), may hold values from 0 to 23, all different within a row; in each aligned block of 6 rows (0 to 5, 6 to 11, ..., all dimensions but the last counted through in order) at most 2 rows name the same one
- norm_gain: bfloat16 [2, 3072], P('pp'), may hold values from 0.5 to 1.5
- router: bfloat16 [2, 3072, 24], P('pp'), may hold values from -0.109375 to 0.109375
- dense_gate: bfloat16 [2, 3072, 6144], P('pp', None, ('ep', 'tp')), may hold values from -0.109375 to 0.109375
- dense_up: bfloat16 [2, 3072, 6144], P('pp', None, ('ep', 'tp')), may hold values from -0.109375 to 0.109375
- dense_down: bfloat16 [2, 6144, 3072], P('pp', ('ep', 'tp')), may hold values from -0.078125 to 0.078125
- expert_gate: bfloat16 [2, 16, 3072, 1024], P('pp', 'ep', None, 'tp'), may hold values from -0.109375 to 0.109375
- expert_up: bfloat16 [2, 16, 3072, 1024], P('pp', 'ep', None, 'tp'), may hold values from -0.109375 to 0.109375
- expert_down: bfloat16 [2, 16, 1024, 3072], P('pp', 'ep', 'tp'), may hold values from -0.1875 to 0.1875
Outputs:
- layer_out: bfloat16 [2, 2, 96, 3072], P('pp', None, 'ep')
The draws below stay inside these ranges and needn't reach their ends.
Inputs may be any that keep to these rules, and one draw needn't show every extreme that they name: `route_ids`: the 8 ids of a token differ. In each layer and microbatch, among the 6 tokens of one ep index no id is named by more than 2 tokens, a bound that some block reaches.
All inputs are finite; a program needn't handle non-finite values.
Results may differ from the reference program's by a relative error of at most 0.008.
Values may be sent and summed in bfloat16 or wider, within the bound.
A program may use at most 128 MiB of HBM per device.

```python
import math
import jax
import jax.numpy as jnp
import numpy as np
from jax import lax

D = 3072
FFE = 1024
DFF = 6144
TOPK = 8
T_EP = 6
N_MB = 2
E = 16
E_ALL = 24
CAP = 2
MB = 96
N_EP = 16


def steps_of(own_key, extent, pieces, least, largest):
    def one(axis_at, parts):
        steps = jax.random.uniform(jax.random.fold_in(jax.random.fold_in(own_key, 6), axis_at), (parts,), jnp.float32, least / len(pieces), largest / len(pieces))
        return jnp.repeat(jnp.exp(steps), extent[axis_at] // parts).reshape((-1,) + (1,) * (len(extent) - axis_at - 1))

    factor_of = one(*pieces[0])
    for cut in pieces[1:]:
        factor_of = factor_of * one(*cut)
    return factor_of


def assign_block(rng, own, number, rows, amount, top, most, skew):
    order = jax.random.permutation(rng, amount)
    heavy_load, common = portions_of(amount, rows * top, most, skew, True), portions_of(amount, rows * top, most, skew, False)
    places = jnp.arange(amount)

    def named(sizes, rotation):
        used = int((sizes > 0).sum())
        fixed = max(1, used // 4)
        shifted = fixed + (places - fixed + rotation * (used - fixed)) % max(1, amount - fixed)
        return jnp.zeros((amount,), jnp.int32).at[order[jnp.where(places < fixed, places, shifted)]].set(jnp.asarray(sizes, jnp.int32))

    sizes = jnp.where(number % 4 == 0, named(heavy_load, number // 4), named(common, number - number // 4 - 1))
    mixed = jax.random.permutation(jax.random.fold_in(own, 3), amount)
    giver, sink = mixed[0:amount // 2 * 2:2], mixed[1:amount // 2 * 2:2]
    room = jnp.minimum(sizes[giver] - 1, most - sizes[sink]) // 2
    room = jnp.where((giver == order[0]) | (sink == order[0]) | (sizes[sink] == 0), 0, jnp.maximum(room, 0))
    shifted = jax.random.randint(jax.random.fold_in(own, 4), (amount // 2,), 0, 1 << 20) % (room + 1)
    sizes = sizes.at[giver].add(-shifted).at[sink].add(shifted)
    members = jnp.searchsorted(jnp.cumsum(sizes), jnp.arange(rows * top), side="right").astype(jnp.int32)
    table = members.reshape(top, rows).T
    table = table[jax.random.permutation(jax.random.fold_in(own, 1), rows)]
    rotation = jax.random.randint(jax.random.fold_in(own, 2), (rows, 1), 0, top)
    return jnp.take_along_axis(table, (jnp.arange(top)[None, :] + rotation) % top, axis=1)


def portions_of(amount, total, limit, lean, full):
    loads = [(1 << 20) // math.isqrt(grade ** lean) + 1 for grade in range(1, amount + 1)]
    largest = limit if full else min(limit, max(-(-total // amount), total * loads[0] // sum(loads)))
    least = 1 if total - largest >= amount - 1 else 0
    holding, rest = [largest] + [least] * (amount - 1), total - largest - least * (amount - 1)
    while rest > 0:
        candidates = [i for i in range(1, amount) if holding[i] < largest] or [i for i in range(1, amount) if holding[i] < limit]
        whole, remaining = sum([loads[i] for i in candidates]), rest
        for i in candidates:
            extra = min(limit - holding[i], max(1, remaining * loads[i] // whole), rest)
            holding[i] = holding[i] + extra
            rest = rest - extra
    return np.array(holding)


def bell_draw(key, shape, scale, limit, shards=(), kind=jnp.bfloat16):
    result = jax.random.normal(key, shape, jnp.float32) * scale
    if len(shards) > 0:
        result = steps_of(key, shape, shards, -0.22, 0.18) * result
    return jnp.clip(result, min=-limit, max=limit).astype(kind)


def setup_inputs(seed: int = 0) -> dict:
    keys = jax.random.split(jax.random.key(seed), 11)
    acts = bell_draw(keys[0], (N_MB, MB, D), 1.0, 6.0, ((1, 16),))
    route_ids_keys = jax.random.split(jax.random.fold_in(keys[1], 1), 2 * N_MB * MB // T_EP)
    route_ids_turns = jax.random.permutation(jax.random.fold_in(keys[1], 3), 2 * N_MB * MB // T_EP)
    route_ids = jax.vmap(lambda own, number: assign_block(jax.random.fold_in(keys[1], 2), own, number, T_EP, E_ALL, TOPK, CAP, 2))(route_ids_keys, route_ids_turns).reshape((2, N_MB, MB, TOPK))
    norm_gain = jnp.clip(1.0 + 0.1 * jax.random.normal(keys[2], (2, D), jnp.float32), 0.5, 1.5).astype(jnp.bfloat16)
    router = bell_draw(keys[3], (2, D, E_ALL), D ** -0.5, 0.109375, ((0, 2),))
    dense_gate = bell_draw(keys[4], (2, D, DFF), D ** -0.5, 0.109375, ((0, 2), (2, 16)))
    dense_up = bell_draw(keys[5], (2, D, DFF), D ** -0.5, 0.109375, ((0, 2), (2, 16)))
    dense_down = bell_draw(keys[6], (2, DFF, D), DFF ** -0.5, 0.078125, ((0, 2), (1, 16)))
    expert_gate = bell_draw(keys[7], (2, E, D, FFE), D ** -0.5, 0.109375, ((0, 2), (1, 16)))
    expert_up = bell_draw(keys[8], (2, E, D, FFE), D ** -0.5, 0.109375, ((0, 2), (1, 16)))
    expert_down = bell_draw(keys[9], (2, E, FFE, D), FFE ** -0.5, 0.1875, ((0, 2), (1, 16)))
    return {"acts": acts, "route_ids": route_ids, "norm_gain": norm_gain, "router": router, "dense_gate": dense_gate, "dense_up": dense_up, "dense_down": dense_down, "expert_gate": expert_gate, "expert_up": expert_up, "expert_down": expert_down}


def normalize(inputs, gain):
    widened = inputs.astype(jnp.float32)
    spread = lax.optimization_barrier(jnp.mean(widened * widened, axis=-1, keepdims=True))
    normed = (widened * lax.rsqrt(spread + 1e-06) * gain.astype(jnp.float32)).astype(jnp.bfloat16)
    return (widened, normed)

def gated_block(inputs, w_gate, w_up, w_down):
    gate_part = jnp.dot(inputs, w_gate, preferred_element_type=jnp.float32)
    up_part = jnp.dot(inputs, w_up, preferred_element_type=jnp.float32)
    hidden = (jax.nn.silu(gate_part) * up_part).astype(jnp.bfloat16)
    return jnp.dot(hidden, w_down, preferred_element_type=jnp.float32)

def choice_weights(normed, route_rows, router_w, n_real):
    n_total = router_w.shape[1]
    gates = jax.nn.sigmoid(jnp.dot(normed, router_w, preferred_element_type=jnp.float32))
    picked = (route_rows[:, :, None] == jnp.arange(n_total, dtype=jnp.int32)[None, None, :]).astype(jnp.float32)
    weights = lax.optimization_barrier(jnp.sum(picked * gates[:, None, :], axis=-1))
    zero_share = lax.optimization_barrier(jnp.sum(jnp.where(route_rows >= n_real, weights, jnp.float32(0.0)), axis=-1))
    return (weights, picked, zero_share)

def layer_ref(inputs, route_rows, gain, router_w, d_gate, d_up, d_down, e_gate, e_up, e_down):
    widened, normed = normalize(inputs, gain)
    n_real = e_gate.shape[0]
    weights, picked, zero_share = choice_weights(normed, route_rows, router_w, n_real)
    coef = jnp.einsum('tk,tke->te', weights, picked[:, :, :n_real], precision=lax.Precision.HIGHEST)
    dense = gated_block(normed, d_gate, d_up, d_down)
    token_count = inputs.shape[0]
    buffer_rows = min(token_count, N_EP * CAP)
    slot_range = jnp.arange(buffer_rows, dtype=jnp.float32)

    def one_expert(expert, total):
        hot = lax.optimization_barrier(jnp.sum((route_rows == expert).astype(jnp.float32), axis=-1))
        position = jnp.cumsum(hot) - hot
        select = hot[None, :] * (position[None, :] == slot_range[:, None]).astype(jnp.float32)
        chosen = jnp.dot(select.astype(jnp.bfloat16), normed, preferred_element_type=jnp.float32).astype(jnp.bfloat16)
        produced = gated_block(chosen, e_gate[expert], e_up[expert], e_down[expert])
        column = lax.dynamic_slice_in_dim(coef, expert, 1, 1)
        return total + jnp.dot(select.T, produced, precision=lax.Precision.HIGHEST) * column
    routed = lax.fori_loop(0, n_real, one_expert, jnp.zeros(widened.shape, jnp.float32))
    return (widened + dense + routed + zero_share[:, None] * normed.astype(jnp.float32)).astype(jnp.bfloat16)

def reference(acts, route_ids, norm_gain, router, dense_gate, dense_up, dense_down, expert_gate, expert_up, expert_down):
    first_section = []
    second_section = []
    for micro in range(N_MB):
        early = layer_ref(acts[micro], route_ids[0, micro], norm_gain[0], router[0], dense_gate[0], dense_up[0], dense_down[0], expert_gate[0], expert_up[0], expert_down[0])
        late = layer_ref(early, route_ids[1, micro], norm_gain[1], router[1], dense_gate[1], dense_up[1], dense_down[1], expert_gate[1], expert_up[1], expert_down[1])
        first_section.append(early)
        second_section.append(late)
    return jnp.stack([jnp.stack(first_section), jnp.stack(second_section)])
```

```python
import functools

import jax
import jax.numpy as jnp
from jax import lax
from jax.experimental import pallas as pl
from jax.experimental.pallas import tpu as pltpu
from jax.sharding import PartitionSpec as P

MESH = pl.DeviceIdType.MESH
F32 = jnp.float32
BF16 = jnp.bfloat16


def divisor_at_most(size, unit, limit):
    best = size
    for step in range(unit, size + 1, unit):
        if size % step == 0 and step <= limit:
            best = step
    return best


class Plan:
    def __init__(self, n_pp, n_ep, n_tp, rows, width, f_expert, f_dense):
        self.n_pp, self.n_ep, self.n_tp = n_pp, n_ep, n_tp
        self.planes = 4 if n_ep % 4 == 0 else 1
        self.depth = n_ep // self.planes
        self.rows = rows
        self.padded = -(-rows // 16) * 16
        self.width = width
        self.total = n_ep * rows
        self.column = self.depth * rows
        self.f_expert, self.f_dense = f_expert, f_dense
        self.n_pieces = 2 if width % 256 == 0 else 1
        self.piece = width // self.n_pieces
        self.n_out = divisor_at_most(self.piece, 128, 512)
        self.chunks = width // self.n_out
        self.per_piece = self.piece // self.n_out
        self.e_step = divisor_at_most(f_expert, 128, 256)
        self.batch = 4 if n_ep % 4 == 0 else 1
        self.peers = self.planes * n_tp - 1


def main_kernel(p, x_ref, hot_ref, gain_ref, router_ref, dg_hbm, du_hbm, dd_hbm, eg_hbm, eu_hbm, ed_hbm,
                out_ref, x_all, hot_all, normed, hot_rows, stage, dg, du, dd, eg, eu, ed, hid_d, hid_e,
                part, recv1, s2, recv2, colf, own_normed, w_sem, x_send, x_fwd, x_recv, h_send, h_fwd, h_recv,
                r1_send, r1_recv, r2_send, r2_recv):
    section = lax.axis_index("pp")
    ep = lax.axis_index("ep")
    tp = lax.axis_index("tp")
    z = ep // p.planes
    q = ep % p.planes
    mine = q * p.depth + z

    loads = {}
    order = [("dg", dg_hbm, dg), ("du", du_hbm, du)]
    for j in range(p.f_expert // p.e_step):
        cols = pl.ds(j * p.e_step, p.e_step)
        order.append((("eg", j), eg_hbm.at[:, cols], eg.at[:, cols]))
        order.append((("eu", j), eu_hbm.at[:, cols], eu.at[:, cols]))
    for c in range(p.chunks):
        cols = pl.ds(c * p.n_out, p.n_out)
        order.append((("dd", c), dd_hbm.at[:, cols], dd.at[:, cols]))
        order.append((("ed", c), ed_hbm.at[:, cols], ed.at[:, cols]))
    for i, (name, src, dst) in enumerate(order):
        loads[name] = pltpu.make_async_copy(src, dst, w_sem.at[i])
        loads[name].start()

    def z_peer(i):
        return lax.rem(z + i, p.depth) * p.planes + q

    def plane_peer(i):
        return z * p.planes + lax.rem(q + i, p.planes)

    barrier = pltpu.get_barrier_semaphore()
    greeted = 0
    for ds in range(p.n_pp):
        for dt in range(p.n_tp):
            targets = [z_peer(i) for i in range(1, p.depth)] if dt == 0 else []
            targets += [plane_peer(i) for i in range(1 if ds == 0 and dt == 0 else 0, p.planes)]
            for target in targets:
                pl.semaphore_signal(
                    barrier, inc=1,
                    device_id={"pp": lax.rem(section + ds, p.n_pp), "ep": target, "tp": lax.rem(tp + dt, p.n_tp)},
                    device_id_type=MESH)
                greeted += 1
    pl.semaphore_wait(barrier, greeted)

    def send(src, dst, send_sem, recv_sem, to_section, to_ep, to_tp):
        pltpu.make_async_remote_copy(
            src_ref=src, dst_ref=dst, send_sem=send_sem, recv_sem=recv_sem,
            device_id={"pp": to_section, "ep": to_ep, "tp": to_tp}, device_id_type=MESH).start()

    def arrived(ref, sem):
        pltpu.make_async_copy(ref, ref, sem).wait()

    def scatter_block(src, buf, send_sem, recv_sem, to_section, include_self):
        for i in range(1, p.depth):
            send(src, buf.at[mine], send_sem, recv_sem.at[mine], to_section, z_peer(i), tp)
        for i in range(0 if include_self else 1, p.planes):
            send(src, buf.at[mine], send_sem, recv_sem.at[mine], to_section, plane_peer(i), tp)

    def forward_blocks(buf, fwd_sem, recv_sem):
        for i in range(1, p.depth):
            block = q * p.depth + lax.rem(z + i, p.depth)
            arrived(buf.at[block], recv_sem.at[block])
            for k in range(1, p.planes):
                send(buf.at[block], buf.at[block], fwd_sem, recv_sem.at[block], section, plane_peer(k), tp)

    def collect_blocks(buf, recv_sem):
        for k in range(1, p.planes):
            column = lax.rem(q + k, p.planes)
            for i in range(p.depth):
                block = column * p.depth + i
                arrived(buf.at[block], recv_sem.at[block])

    n_own = p.depth - 1 + p.planes - 1
    n_fwd = (p.depth - 1) * (p.planes - 1)

    @pl.when(section == 0)
    def _():
        for a in range(p.n_pieces):
            scatter_block(x_ref.at[a], x_all.at[a], x_send.at[a], x_recv.at[a], section, False)
            x_all[a, mine] = x_ref[a]

    scatter_block(hot_ref, hot_all, h_send, h_recv, section, False)
    hot_all[mine] = hot_ref[...]
    s2[...] = jnp.zeros_like(s2)

    @pl.when(section == 0)
    def _():
        for a in range(p.n_pieces):
            forward_blocks(x_all.at[a], x_fwd.at[a], x_recv.at[a])

    forward_blocks(hot_all, h_fwd, h_recv)
    collect_blocks(hot_all, h_recv)

    @pl.when(section > 0)
    def _():
        for a in range(p.n_pieces):
            arrived(x_all.at[a, mine], x_recv.at[a, mine])
            forward_blocks(x_all.at[a], x_fwd.at[a], x_recv.at[a])

    for a in range(p.n_pieces):
        collect_blocks(x_all.at[a], x_recv.at[a])

    gain = gain_ref[...].astype(F32)

    def inverse_spread(block):
        total = 0.0
        for a in range(p.n_pieces):
            v = x_all[a, block].astype(F32)
            total = total + jnp.sum(v * v, axis=-1, keepdims=True)
        return lax.rsqrt(total / p.width + 1e-06)

    def norm_body(k, _):
        for i in range(p.batch):
            block = k * p.batch + i
            inv = inverse_spread(block)
            low = i * p.rows
            for a in range(p.n_pieces):
                v = x_all[a, block].astype(F32) * inv * gain[:, a * p.piece:(a + 1) * p.piece]
                stage[low:low + p.rows, a * p.piece:(a + 1) * p.piece] = v[:p.rows]
            stage[low:low + p.rows, p.width:] = hot_all[block].astype(F32)[:p.rows]
        height = p.batch * p.rows
        at = pl.ds(pl.multiple_of(k * height, height), height)
        normed[at, :] = stage[:, :p.width].astype(BF16)
        hot_rows[at, :] = stage[:, p.width:]
        return 0

    lax.fori_loop(0, p.n_ep // p.batch, norm_body, 0)

    def gates_of(rows):
        return jax.nn.sigmoid(jnp.dot(rows, router_ref[...], preferred_element_type=F32))

    n_ids = router_ref.shape[1]
    gates = gates_of(normed[...])
    lane = lax.broadcasted_iota(jnp.int32, (p.total, n_ids), 1)
    coef = jnp.sum(jnp.where(lane == ep, gates * hot_rows[...][:, :n_ids], 0.0), axis=-1, keepdims=True)

    def hidden_of(w_gate, w_up):
        g = jnp.dot(normed[...], w_gate, preferred_element_type=F32)
        u = jnp.dot(normed[...], w_up, preferred_element_type=F32)
        return g * jax.nn.sigmoid(g) * u

    loads["dg"].wait()
    loads["du"].wait()
    hid_d[...] = hidden_of(dg[...], du[...]).astype(BF16)
    for j in range(p.f_expert // p.e_step):
        loads["eg", j].wait()
        loads["eu", j].wait()
        cols = slice(j * p.e_step, (j + 1) * p.e_step)
        hid_e[:, cols] = (hidden_of(eg[:, cols], eu[:, cols]) * coef).astype(BF16)

    for c in range(p.chunks):
        loads["dd", c].wait()
        loads["ed", c].wait()
        cols = slice(c * p.n_out, (c + 1) * p.n_out)
        value = jnp.dot(hid_e[...], ed[:, cols], preferred_element_type=F32)
        value += jnp.dot(hid_d[...], dd[:, cols], preferred_element_type=F32)
        part[c] = value.astype(BF16)
        for dt in range(p.n_tp):
            for k in range(0 if dt else 1, p.planes):
                column = lax.rem(q + k, p.planes)
                at = pl.ds(pl.multiple_of(column * p.column, p.column), p.column)
                send(part.at[c, at], recv1.at[c, dt * p.planes + k - 1], r1_send, r1_recv.at[c],
                     section, plane_peer(k), lax.rem(tp + dt, p.n_tp))

    inv = inverse_spread(mine)
    for a in range(p.n_pieces):
        cols = slice(a * p.piece, (a + 1) * p.piece)
        own_normed[:, cols] = (x_all[a, mine].astype(F32) * inv * gain[:, cols]).astype(BF16)
    own_gates = gates_of(own_normed[...])
    own_lane = lax.broadcasted_iota(jnp.int32, own_gates.shape, 1)
    own_hot = hot_ref[...].astype(F32)[:, :n_ids]
    zero_share = jnp.sum(jnp.where(own_lane >= p.n_ep, own_gates * own_hot, 0.0), axis=-1, keepdims=True)

    own_rows = pl.ds(pl.multiple_of(q * p.column, p.column), p.column)
    for c in range(p.chunks):
        acc = part[c, own_rows].astype(F32)
        if p.peers:
            arrived(recv1.at[c], r1_recv.at[c])
            for k in range(p.peers):
                acc += recv1[c, k].astype(F32)
        colf[...] = acc
        for i in range(p.depth):
            s2[c, i, :p.rows] = colf[i * p.rows:(i + 1) * p.rows].astype(BF16)
        for i in range(1, p.depth):
            send(s2.at[c, lax.rem(z + i, p.depth)], recv2.at[c, i - 1], r2_send, r2_recv.at[c],
                 section, z_peer(i), tp)

    for c in range(p.chunks):
        a, inner = c // p.per_piece, c % p.per_piece
        cols = slice(inner * p.n_out, (inner + 1) * p.n_out)
        acc = s2[c, z].astype(F32)
        arrived(recv2.at[c], r2_recv.at[c])
        for k in range(p.depth - 1):
            acc += recv2[c, k].astype(F32)
        acc += x_all[a, mine, :, cols].astype(F32)
        acc += zero_share * own_normed[:, c * p.n_out:(c + 1) * p.n_out].astype(F32)
        out_ref[a, :, cols] = acc.astype(BF16)
        if inner == p.per_piece - 1:
            @pl.when(section < p.n_pp - 1)
            def _():
                scatter_block(out_ref.at[a], x_all.at[a], x_send.at[p.n_pieces + a], x_recv.at[a],
                              section + 1, True)

    arrived(hot_all.at[pl.ds(0, n_own)], h_send)
    arrived(hot_all.at[pl.ds(0, n_fwd)], h_fwd)
    for a in range(p.n_pieces):
        arrived(x_all.at[a, pl.ds(0, n_fwd)], x_fwd.at[a])
    if p.peers:
        arrived(recv1, r1_send)
    arrived(recv2, r2_send)

    @pl.when(section == 0)
    def _():
        for a in range(p.n_pieces):
            arrived(x_all.at[a, pl.ds(0, n_own)], x_send.at[a])

    @pl.when(section < p.n_pp - 1)
    def _():
        for a in range(p.n_pieces):
            arrived(x_all.at[a, pl.ds(0, n_own + 1)], x_send.at[p.n_pieces + a])


def on_device(sizes, acts, route_ids, norm_gain, router, dense_gate, dense_up, dense_down,
              expert_gate, expert_up, expert_down):
    n_pp, n_ep, n_tp = sizes
    n_micro, per_group, width = acts.shape
    rows = n_micro * per_group
    f_expert, f_dense = expert_gate.shape[-1], dense_gate.shape[-1]
    p = Plan(n_pp, n_ep, n_tp, rows, width, f_expert, f_dense)
    n_ids = router.shape[-1]
    lanes = -(-n_ids // 128) * 128

    x = jnp.pad(acts.reshape(rows, width), ((0, p.padded - rows), (0, 0)))
    x = x.reshape(p.padded, p.n_pieces, p.piece).transpose(1, 0, 2)
    ids = route_ids[0].reshape(rows, -1)
    hot = jnp.sum((ids[:, :, None] == jnp.arange(lanes, dtype=jnp.int32)).astype(F32), axis=1).astype(BF16)
    hot = jnp.pad(hot, ((0, p.padded - rows), (0, 0)))

    vmem = pl.BlockSpec(memory_space=pltpu.VMEM)
    hbm = pl.BlockSpec(memory_space=pl.ANY)
    dma = pltpu.SemaphoreType.DMA
    n_loads = 2 + 2 * (f_expert // p.e_step) + 2 * p.chunks
    out = pl.pallas_call(
        functools.partial(main_kernel, p),
        out_shape=jax.ShapeDtypeStruct((p.n_pieces, p.padded, p.piece), BF16),
        in_specs=[vmem] * 4 + [hbm] * 6,
        out_specs=vmem,
        scratch_shapes=[
            pltpu.VMEM((p.n_pieces, n_ep, p.padded, p.piece), BF16),
            pltpu.VMEM((n_ep, p.padded, lanes), BF16),
            pltpu.VMEM((p.total, width), BF16),
            pltpu.VMEM((p.total, lanes), F32),
            pltpu.VMEM((p.batch * rows, width + lanes), F32),
            pltpu.VMEM((width, f_dense), BF16),
            pltpu.VMEM((width, f_dense), BF16),
            pltpu.VMEM((f_dense, width), BF16),
            pltpu.VMEM((width, f_expert), BF16),
            pltpu.VMEM((width, f_expert), BF16),
            pltpu.VMEM((f_expert, width), BF16),
            pltpu.VMEM((p.total, f_dense), BF16),
            pltpu.VMEM((p.total, f_expert), BF16),
            pltpu.VMEM((p.chunks, p.total, p.n_out), BF16),
            pltpu.VMEM((p.chunks, max(p.peers, 1), p.column, p.n_out), BF16),
            pltpu.VMEM((p.chunks, p.depth, p.padded, p.n_out), BF16),
            pltpu.VMEM((p.chunks, p.depth - 1, p.padded, p.n_out), BF16),
            pltpu.VMEM((p.column, p.n_out), F32),
            pltpu.VMEM((p.padded, width), BF16),
            dma((n_loads,)),
            dma((2 * p.n_pieces,)),
            dma((p.n_pieces,)),
            dma((p.n_pieces, n_ep)),
            dma, dma, dma((n_ep,)),
            dma, dma((p.chunks,)),
            dma, dma((p.chunks,)),
        ],
        compiler_params=pltpu.CompilerParams(
            collective_id=0, has_side_effects=True, vmem_limit_bytes=60 * 1024 * 1024),
    )(x, hot, norm_gain, router[0], dense_gate[0], dense_up[0], dense_down[0],
      expert_gate[0, 0], expert_up[0, 0], expert_down[0, 0])
    out = out.transpose(1, 0, 2).reshape(p.padded, width)[:rows]
    return out.reshape(1, n_micro, per_group, width)


def solution(mesh):
    sizes = (mesh.shape["pp"], mesh.shape["ep"], mesh.shape["tp"])
    return jax.shard_map(
        functools.partial(on_device, sizes),
        mesh=mesh,
        in_specs=(
            P(None, "ep", None),
            P("pp", None, "ep", None),
            P("pp", None),
            P("pp", None, None),
            P("pp", None, ("ep", "tp")),
            P("pp", None, ("ep", "tp")),
            P("pp", ("ep", "tp"), None),
            P("pp", "ep", None, "tp"),
            P("pp", "ep", None, "tp"),
            P("pp", "ep", "tp", None),
        ),
        out_specs=P("pp", None, "ep", None),
        check_vma=False,
    )
```

```python
import functools

import jax
import jax.numpy as jnp
from jax import lax
from jax.experimental import pallas as pl
from jax.experimental.pallas import tpu as pltpu
from jax.sharding import PartitionSpec as P

MESH = pl.DeviceIdType.MESH
F32 = jnp.float32
BF16 = jnp.bfloat16


def divisor_at_most(size, unit, limit):
    best = size
    for step in range(unit, size + 1, unit):
        if size % step == 0 and step <= limit:
            best = step
    return best


class Plan:
    def __init__(self, n_pp, n_ep, n_tp, rows, width, f_expert, f_dense):
        self.n_pp, self.n_ep, self.n_tp = n_pp, n_ep, n_tp
        self.planes = 4 if n_ep % 4 == 0 else 1
        self.depth = n_ep // self.planes
        self.rows = rows
        self.padded = -(-rows // 16) * 16
        self.width = width
        self.total = n_ep * rows
        self.column = self.depth * rows
        self.f_expert, self.f_dense = f_expert, f_dense
        self.n_out = divisor_at_most(width, 128, 512)
        self.chunks = width // self.n_out
        spare = self.padded - rows
        self.tails = rows // spare if spare and rows % spare == 0 else 0
        self.spare = spare
        if self.n_out % (128 * (self.tails + 1)):
            self.tails = 0
        self.tail = self.n_out // (self.tails + 1) if self.tails else 0
        self.main = self.n_out - self.tail
        self.e_step = divisor_at_most(f_expert, 128, 256)
        self.batch = 4 if n_ep % 4 == 0 else 1
        self.peers = self.planes * n_tp - 1


def main_kernel(p, x_ref, ids_ref, gain_ref, router_ref, dg_hbm, du_hbm, dd_hbm, eg_hbm, eu_hbm, ed_hbm,
                out_ref, x_all, hot_all, normed, hot_rows, stage, dg, du, dd, eg, eu, ed, hid_d, hid_e,
                part, recv1, s2, recv2, colf, own_normed, own_x, own_hot, tile, packed, x_own, x_next, hot_own, w_sem, x_send, x_fwd, x_recv, h_send, h_fwd, h_recv,
                r1_send, r1_recv, r2_send, r2_recv):
    section = lax.axis_index("pp")
    ep = lax.axis_index("ep")
    tp = lax.axis_index("tp")
    z = ep // p.planes
    q = ep % p.planes
    mine = q * p.depth + z

    loads = {}
    order = [("dg", dg_hbm, dg), ("du", du_hbm, du)]
    for j in range(p.f_expert // p.e_step):
        cols = pl.ds(j * p.e_step, p.e_step)
        order.append((("eg", j), eg_hbm.at[:, cols], eg.at[:, cols]))
        order.append((("eu", j), eu_hbm.at[:, cols], eu.at[:, cols]))
    for c in range(p.chunks):
        cols = pl.ds(c * p.n_out, p.n_out)
        order.append((("dd", c), dd_hbm.at[:, cols], dd.at[:, cols]))
        order.append((("ed", c), ed_hbm.at[:, cols], ed.at[:, cols]))
    for i, (name, src, dst) in enumerate(order):
        loads[name] = pltpu.make_async_copy(src, dst, w_sem.at[i])
        loads[name].start()

    micro = x_ref.shape[1]
    n_ids = router_ref.shape[0]

    def unpack(block, dst, low):
        for c in range(p.chunks):
            v = x_all[c, block].astype(F32)
            left = c * p.n_out
            dst[low:low + p.rows, left:left + p.main] = v[:p.rows]
            for j in range(p.tails):
                dst[low + j * p.spare:low + (j + 1) * p.spare, left + p.main:left + p.n_out] = (
                    v[p.rows:, j * p.tail:(j + 1) * p.tail])

    def pack(src, left, c, dst):
        packed[:p.rows, :] = src[:p.rows, left:left + p.main]
        for j in range(p.tails):
            packed[p.rows:, j * p.tail:(j + 1) * p.tail] = (
                src[j * p.spare:(j + 1) * p.spare, left + p.main:left + p.n_out])
        dst[c] = packed[...].astype(BF16)

    own_x[...] = jnp.zeros_like(own_x)
    own_hot[...] = jnp.zeros_like(own_hot)
    packed[...] = jnp.zeros_like(packed)
    for t in range(x_ref.shape[0]):
        low = t * micro
        own_x[low:low + micro, :] = x_ref[t].astype(F32)
        ids = ids_ref[t]
        lanes = lax.broadcasted_iota(jnp.int32, (micro, own_hot.shape[1]), 1)
        named = jnp.zeros(lanes.shape, F32)
        for k in range(ids.shape[1]):
            named += (ids[:, k:k + 1] == lanes).astype(F32)
        own_hot[low:low + micro, :] = named
    hot_own[...] = own_hot[...].astype(BF16)

    @pl.when(section == 0)
    def _():
        for c in range(p.chunks):
            pack(own_x, c * p.n_out, c, x_own)

    def z_peer(i):
        return lax.rem(z + i, p.depth) * p.planes + q

    def plane_peer(i):
        return z * p.planes + lax.rem(q + i, p.planes)

    barrier = pltpu.get_barrier_semaphore()
    greeted = 0
    for ds in range(p.n_pp):
        for dt in range(p.n_tp):
            targets = [z_peer(i) for i in range(1, p.depth)] if dt == 0 else []
            targets += [plane_peer(i) for i in range(1 if ds == 0 and dt == 0 else 0, p.planes)]
            for target in targets:
                pl.semaphore_signal(
                    barrier, inc=1,
                    device_id={"pp": lax.rem(section + ds, p.n_pp), "ep": target, "tp": lax.rem(tp + dt, p.n_tp)},
                    device_id_type=MESH)
                greeted += 1
    pl.semaphore_wait(barrier, greeted)

    def send(src, dst, send_sem, recv_sem, to_section, to_ep, to_tp):
        pltpu.make_async_remote_copy(
            src_ref=src, dst_ref=dst, send_sem=send_sem, recv_sem=recv_sem,
            device_id={"pp": to_section, "ep": to_ep, "tp": to_tp}, device_id_type=MESH).start()

    def arrived(ref, sem):
        pltpu.make_async_copy(ref, ref, sem).wait()

    def scatter_block(src, buf, send_sem, recv_sem, to_section, include_self):
        for i in range(1, p.depth):
            send(src, buf.at[mine], send_sem, recv_sem.at[z], to_section, z_peer(i), tp)
        for i in range(1, p.planes):
            send(src, buf.at[mine], send_sem, recv_sem.at[p.depth], to_section, plane_peer(i), tp)
        if include_self:
            send(src, buf.at[mine], send_sem, recv_sem.at[z], to_section, ep, tp)

    def forward_blocks(buf, fwd_sem, recv_sem):
        for i in range(1, p.depth):
            source = lax.rem(z + i, p.depth)
            block = q * p.depth + source
            arrived(buf.at[block], recv_sem.at[source])
            for k in range(1, p.planes):
                send(buf.at[block], buf.at[block], fwd_sem, recv_sem.at[p.depth], section, plane_peer(k), tp)

    def collect_blocks(buf, recv_sem):
        if p.planes > 1:
            arrived(buf.at[pl.ds(0, (p.planes - 1) * p.depth)], recv_sem.at[p.depth])

    n_own = p.depth - 1 + p.planes - 1
    n_fwd = (p.depth - 1) * (p.planes - 1)

    @pl.when(section == 0)
    def _():
        for a in range(p.chunks):
            scatter_block(x_own.at[a], x_all.at[a], x_send.at[a], x_recv.at[a], section, False)
            x_all[a, mine] = x_own[a]

    scatter_block(hot_own, hot_all, h_send, h_recv, section, False)
    hot_all[mine] = hot_own[...]
    s2[...] = jnp.zeros_like(s2)

    @pl.when(section == 0)
    def _():
        for a in range(p.chunks):
            forward_blocks(x_all.at[a], x_fwd.at[a], x_recv.at[a])

    forward_blocks(hot_all, h_fwd, h_recv)
    collect_blocks(hot_all, h_recv)

    @pl.when(section > 0)
    def _():
        for a in range(p.chunks):
            arrived(x_all.at[a, mine], x_recv.at[a, z])
            forward_blocks(x_all.at[a], x_fwd.at[a], x_recv.at[a])

    for a in range(p.chunks):
        collect_blocks(x_all.at[a], x_recv.at[a])

    gain = gain_ref[...].astype(F32)

    def rms_normed(v):
        spread = jnp.mean(v * v, axis=-1, keepdims=True)
        return (v * lax.rsqrt(spread + 1e-06) * gain).astype(BF16)

    def norm_body(k, _):
        for i in range(p.batch):
            block = k * p.batch + i
            low = i * p.rows
            unpack(block, stage, low)
            stage[low:low + p.rows, p.width:] = hot_all[block].astype(F32)[:p.rows]
        height = p.batch * p.rows
        at = pl.ds(pl.multiple_of(k * height, height), height)
        normed[at, :] = rms_normed(stage[:, :p.width])
        hot_rows[at, :] = stage[:, p.width:]
        return 0

    lax.fori_loop(0, p.n_ep // p.batch, norm_body, 0)

    def gates_of(rows):
        return jax.nn.sigmoid(lax.dot_general(
            rows, router_ref[...], (((1,), (1,)), ((), ())), preferred_element_type=F32))

    gates = gates_of(normed[...])
    lane = lax.broadcasted_iota(jnp.int32, (p.total, n_ids), 1)
    coef = jnp.sum(jnp.where(lane == ep, gates * hot_rows[...][:, :n_ids], 0.0), axis=-1, keepdims=True)

    def hidden_of(w_gate, w_up):
        g = jnp.dot(normed[...], w_gate, preferred_element_type=F32)
        u = jnp.dot(normed[...], w_up, preferred_element_type=F32)
        return g * jax.nn.sigmoid(g) * u

    loads["dg"].wait()
    loads["du"].wait()
    hid_d[...] = hidden_of(dg[...], du[...]).astype(BF16)
    for j in range(p.f_expert // p.e_step):
        loads["eg", j].wait()
        loads["eu", j].wait()
        cols = slice(j * p.e_step, (j + 1) * p.e_step)
        hid_e[:, cols] = (hidden_of(eg[:, cols], eu[:, cols]) * coef).astype(BF16)

    for c in range(p.chunks):
        loads["dd", c].wait()
        loads["ed", c].wait()
        cols = slice(c * p.n_out, (c + 1) * p.n_out)
        value = jnp.dot(hid_e[...], ed[:, cols], preferred_element_type=F32)
        value += jnp.dot(hid_d[...], dd[:, cols], preferred_element_type=F32)
        part[c] = value.astype(BF16)
        for dt in range(p.n_tp):
            for k in range(0 if dt else 1, p.planes):
                column = lax.rem(q + k, p.planes)
                at = pl.ds(pl.multiple_of(column * p.column, p.column), p.column)
                send(part.at[c, at], recv1.at[c, dt * p.planes + k - 1], r1_send, r1_recv.at[c],
                     section, plane_peer(k), lax.rem(tp + dt, p.n_tp))

    unpack(mine, own_x, 0)
    own_normed[...] = rms_normed(own_x[...])
    own_gates = gates_of(own_normed[...])
    own_lane = lax.broadcasted_iota(jnp.int32, own_gates.shape, 1)
    own_named = own_hot[...][:, :n_ids]
    zero_share = jnp.sum(jnp.where(own_lane >= p.n_ep, own_gates * own_named, 0.0), axis=-1, keepdims=True)

    own_rows = pl.ds(pl.multiple_of(q * p.column, p.column), p.column)
    for c in range(p.chunks):
        acc = part[c, own_rows].astype(F32)
        if p.peers:
            arrived(recv1.at[c], r1_recv.at[c])
            for k in range(p.peers):
                acc += recv1[c, k].astype(F32)
        colf[...] = acc
        for i in range(p.depth):
            s2[c, i, :p.rows] = colf[i * p.rows:(i + 1) * p.rows].astype(BF16)
        for i in range(1, p.depth):
            send(s2.at[c, lax.rem(z + i, p.depth)], recv2.at[c, i - 1], r2_send, r2_recv.at[c],
                 section, z_peer(i), tp)

    for c in range(p.chunks):
        cols = slice(c * p.n_out, (c + 1) * p.n_out)
        acc = s2[c, z].astype(F32)
        arrived(recv2.at[c], r2_recv.at[c])
        for k in range(p.depth - 1):
            acc += recv2[c, k].astype(F32)
        acc += own_x[:, cols]
        acc += zero_share * own_normed[:, cols].astype(F32)
        tile[...] = acc
        if p.n_pp > 1:
            @pl.when(section < p.n_pp - 1)
            def _():
                pack(tile, 0, c, x_next)
                scatter_block(x_next.at[c], x_all.at[c], x_send.at[p.chunks + c], x_recv.at[c],
                              section + 1, True)
        for t in range(x_ref.shape[0]):
            out_ref[t, :, cols] = tile[t * micro:(t + 1) * micro, :].astype(BF16)

    arrived(hot_all.at[pl.ds(0, n_own)], h_send)
    arrived(hot_all.at[pl.ds(0, n_fwd)], h_fwd)
    for a in range(p.chunks):
        arrived(x_all.at[a, pl.ds(0, n_fwd)], x_fwd.at[a])
    if p.peers:
        arrived(recv1, r1_send)
    arrived(recv2, r2_send)

    @pl.when(section == 0)
    def _():
        for a in range(p.chunks):
            arrived(x_all.at[a, pl.ds(0, n_own)], x_send.at[a])

    @pl.when(section < p.n_pp - 1)
    def _():
        for a in range(p.chunks):
            arrived(x_all.at[a, pl.ds(0, n_own + 1)], x_send.at[p.chunks + a])


def on_device(sizes, acts, route_ids, norm_gain, router, dense_gate, dense_up, dense_down,
              expert_gate, expert_up, expert_down):
    n_pp, n_ep, n_tp = sizes
    n_micro, per_group, width = acts.shape
    rows = n_micro * per_group
    f_expert, f_dense = expert_gate.shape[-1], dense_gate.shape[-1]
    p = Plan(n_pp, n_ep, n_tp, rows, width, f_expert, f_dense)
    n_ids = router.shape[-1]
    lanes = -(-n_ids // 128) * 128

    x = acts.transpose(1, 0, 2)
    ids = route_ids[0].transpose(1, 0, 2)

    vmem = pl.BlockSpec(memory_space=pltpu.VMEM)
    hbm = pl.BlockSpec(memory_space=pl.ANY)
    dma = pltpu.SemaphoreType.DMA
    n_loads = 2 + 2 * (f_expert // p.e_step) + 2 * p.chunks
    out = pl.pallas_call(
        functools.partial(main_kernel, p),
        out_shape=jax.ShapeDtypeStruct((per_group, n_micro, width), BF16),
        in_specs=[vmem] * 4 + [hbm] * 6,
        out_specs=vmem,
        scratch_shapes=[
            pltpu.VMEM((p.chunks, n_ep, p.padded, p.main), BF16),
            pltpu.VMEM((n_ep, p.padded, lanes), BF16),
            pltpu.VMEM((p.total, width), BF16),
            pltpu.VMEM((p.total, lanes), F32),
            pltpu.VMEM((p.batch * rows, width + lanes), F32),
            pltpu.VMEM((width, f_dense), BF16),
            pltpu.VMEM((width, f_dense), BF16),
            pltpu.VMEM((f_dense, width), BF16),
            pltpu.VMEM((width, f_expert), BF16),
            pltpu.VMEM((width, f_expert), BF16),
            pltpu.VMEM((f_expert, width), BF16),
            pltpu.VMEM((p.total, f_dense), BF16),
            pltpu.VMEM((p.total, f_expert), BF16),
            pltpu.VMEM((p.chunks, p.total, p.n_out), BF16),
            pltpu.VMEM((p.chunks, max(p.peers, 1), p.column, p.n_out), BF16),
            pltpu.VMEM((p.chunks, p.depth, p.padded, p.n_out), BF16),
            pltpu.VMEM((p.chunks, p.depth - 1, p.padded, p.n_out), BF16),
            pltpu.VMEM((p.column, p.n_out), F32),
            pltpu.VMEM((p.padded, width), BF16),
            pltpu.VMEM((p.padded, width), F32),
            pltpu.VMEM((p.padded, lanes), F32),
            pltpu.VMEM((p.padded, p.n_out), F32),
            pltpu.VMEM((p.padded, p.main), F32),
            pltpu.VMEM((p.chunks, p.padded, p.main), BF16),
            pltpu.VMEM((p.chunks, p.padded, p.main), BF16),
            pltpu.VMEM((p.padded, lanes), BF16),
            dma((n_loads,)),
            dma((2 * p.chunks,)),
            dma((p.chunks,)),
            dma((p.chunks, p.depth + 1)),
            dma, dma, dma((p.depth + 1,)),
            dma, dma((p.chunks,)),
            dma, dma((p.chunks,)),
        ],
        compiler_params=pltpu.CompilerParams(
            collective_id=0, has_side_effects=True, vmem_limit_bytes=60 * 1024 * 1024),
    )(x, ids, norm_gain, router[0].T, dense_gate[0], dense_up[0], dense_down[0],
      expert_gate[0, 0], expert_up[0, 0], expert_down[0, 0])
    return out.transpose(1, 0, 2)[None]


def solution(mesh):
    sizes = (mesh.shape["pp"], mesh.shape["ep"], mesh.shape["tp"])
    return jax.shard_map(
        functools.partial(on_device, sizes),
        mesh=mesh,
        in_specs=(
            P(None, "ep", None),
            P("pp", None, "ep", None),
            P("pp", None),
            P("pp", None, None),
            P("pp", None, ("ep", "tp")),
            P("pp", None, ("ep", "tp")),
            P("pp", ("ep", "tp"), None),
            P("pp", "ep", None, "tp"),
            P("pp", "ep", None, "tp"),
            P("pp", "ep", "tp", None),
        ),
        out_specs=P("pp", None, "ep", None),
        check_vma=False,
    )
```
